16 devices in a mesh: sp: 16 (over z, y, x, core).
Axes of the slice: x: 2, y: 2, z: 2, core: 2. Of those that a mesh axis runs over, the one named last changes fastest.
Arguments:
- x: bfloat16 [3, 4096, 2048], P(None, 'sp')
- ln1_w: bfloat16 [2048], replicated
- w_qkv: bfloat16 [2048, 6144], replicated
- q_ln_w: bfloat16 [16, 128], replicated
- k_ln_w: bfloat16 [16, 128], replicated
- w_out: bfloat16 [2048, 2048], replicated
- grad_y: bfloat16 [3, 4096, 2048], P(None, 'sp')
Outputs:
- output 1: bfloat16 [3, 4096, 2048], P(None, 'sp')
- output 2: bfloat16 [3, 4096, 2048], P(None, 'sp')
- output 3: float32 [2048], replicated
- output 4: float32 [2048, 6144], replicated
- output 5: float32 [16, 128], replicated
- output 6: float32 [16, 128], replicated
- output 7: float32 [2048, 2048], replicated
All inputs are finite; a program needn't handle non-finite values.
Results may differ from the reference program's by a relative error of at most 0.0129169.
Values are sent between devices in bfloat16 or wider.
A program may use at most 1 GiB of HBM per device.

```python
import math
import jax
import jax.numpy as jnp
from jax import lax

BATCH_SIZE = 3
SEQ_LEN = 4096
D_MODEL = 2048
N_HEADS = 16
HEAD_DIM = 128
Q_BLOCK = math.gcd(SEQ_LEN, 256)


def alibi_slopes(n_heads):
    pow_two = 2 ** math.ceil(math.log2(n_heads))
    exponents = jnp.arange(1, pow_two + 1, dtype=jnp.float32) * (8.0 / pow_two)
    slopes = jnp.exp2(-exponents)
    if pow_two != n_heads:
        slopes = jnp.concatenate([slopes[1::2], slopes[0::2]])[:n_heads]
    return slopes


def layer_norm(values, weight):
    centered = values - jnp.mean(values, axis=-1, keepdims=True)
    var_val = jnp.mean(centered * centered, axis=-1, keepdims=True)
    return centered * lax.rsqrt(var_val + 1e-5) * weight


def bf_cast(values):
    return values.astype(jnp.bfloat16).astype(jnp.float32)


def setup_inputs(seed: int = 0) -> dict:
    key_list = jax.random.split(jax.random.key(seed), 8)
    act_shape = (BATCH_SIZE, SEQ_LEN, D_MODEL)
    w_scale = D_MODEL ** -0.5
    head_gain = jnp.exp2(jax.random.uniform(key_list[3], (N_HEADS, 1), jnp.float32, -1.0, 1.0))
    q_gain = (1.0 + 0.3 * jax.random.normal(key_list[4], (N_HEADS, HEAD_DIM), jnp.float32)) * head_gain
    return {
        'x': jax.random.normal(key_list[0], act_shape, jnp.float32).astype(jnp.bfloat16),
        'ln1_w': (1.0 + 0.3 * jax.random.normal(key_list[1], (D_MODEL,), jnp.float32)).astype(jnp.bfloat16),
        'w_qkv': (jax.random.normal(key_list[2], (D_MODEL, 3 * D_MODEL), jnp.float32) * w_scale).astype(jnp.bfloat16),
        'q_ln_w': q_gain.astype(jnp.bfloat16),
        'k_ln_w': (1.0 + 0.3 * jax.random.normal(key_list[5], (N_HEADS, HEAD_DIM), jnp.float32)).astype(jnp.bfloat16),
        'w_out': (jax.random.normal(key_list[6], (D_MODEL, D_MODEL), jnp.float32) * w_scale).astype(jnp.bfloat16),
        'grad_y': jax.random.normal(key_list[7], act_shape, jnp.float32).astype(jnp.bfloat16),
    }


def head_attention(head_args):
    q_head, k_head, v_head, head_slope = head_args
    key_pos = jnp.arange(SEQ_LEN)

    def block_attention(blk_idx):
        q_part = lax.dynamic_slice_in_dim(q_head, blk_idx * Q_BLOCK, Q_BLOCK, axis=1)
        scores = jnp.einsum('bqd,bkd->bqk', q_part, k_head) * (HEAD_DIM ** -0.5)
        pos_gap = (blk_idx * Q_BLOCK + jnp.arange(Q_BLOCK))[:, None] - key_pos[None, :]
        scores = jnp.where(pos_gap >= 0, scores - head_slope * pos_gap.astype(jnp.float32), -1e30)
        row_max = lax.stop_gradient(jnp.max(scores, axis=-1, keepdims=True))
        weights = jnp.exp(scores - row_max)
        weighted = jnp.einsum('bqk,bkd->bqd', weights, v_head)
        return weighted / jnp.sum(weights, axis=-1, keepdims=True)

    out_blocks = lax.map(jax.checkpoint(block_attention), jnp.arange(SEQ_LEN // Q_BLOCK))
    return jnp.moveaxis(out_blocks, 0, 1).reshape(BATCH_SIZE, SEQ_LEN, HEAD_DIM)


def forward_pass(x, ln1_w, w_qkv, q_ln_w, k_ln_w, w_out):
    h_act = bf_cast(layer_norm(x, ln1_w))
    qkv_raw = jnp.einsum('bsd,de->bse', h_act, w_qkv)
    q_all = bf_cast(layer_norm(qkv_raw[..., :D_MODEL], q_ln_w.reshape(D_MODEL)))
    k_all = bf_cast(layer_norm(qkv_raw[..., D_MODEL:2 * D_MODEL], k_ln_w.reshape(D_MODEL)))
    v_all = bf_cast(qkv_raw[..., 2 * D_MODEL:])
    head_shape = (BATCH_SIZE, SEQ_LEN, N_HEADS, HEAD_DIM)
    per_head = [jnp.moveaxis(tensor.reshape(head_shape), 2, 0) for tensor in (q_all, k_all, v_all)]
    o_heads = lax.map(jax.checkpoint(head_attention), (per_head[0], per_head[1], per_head[2], alibi_slopes(N_HEADS)))
    o_all = bf_cast(jnp.moveaxis(o_heads, 0, 2).reshape(BATCH_SIZE, SEQ_LEN, D_MODEL))
    return jnp.einsum('bsd,de->bse', o_all, w_out) + x


def reference(x, ln1_w, w_qkv, q_ln_w, k_ln_w, w_out, grad_y):
    y_val, pull_back = jax.vjp(forward_pass, x.astype(jnp.float32), ln1_w.astype(jnp.float32), w_qkv.astype(jnp.float32), q_ln_w.astype(jnp.float32), k_ln_w.astype(jnp.float32), w_out.astype(jnp.float32))
    grad_list = pull_back(grad_y.astype(jnp.float32))
    return (y_val.astype(jnp.bfloat16), grad_list[0].astype(jnp.bfloat16), grad_list[1], grad_list[2], grad_list[3], grad_list[4], grad_list[5])
```

```python
import functools, math
import jax
import jax.numpy as jnp
from jax import lax
from jax.experimental import pallas as pl
from jax.experimental.pallas import tpu as pltpu
from jax.sharding import PartitionSpec as P

def attn_kernel(blk, tok, slope_ref, q_ref, k_ref, v_ref, do_ref, out_ref, kt_ref, vt_ref, s_ref, dp_ref, dk_ref, dv_ref, acc_ref):
    i = pl.program_id(0)
    n_blk = pl.num_programs(0)
    head_dim = q_ref.shape[1]
    f32, bf16 = jnp.float32, jnp.bfloat16
    scale = head_dim ** -0.5
    log2e = math.log2(math.e)
    slope2 = slope_ref[0] * log2e
    nt = (((1,), (1,)), ((), ()))

    def rows(j):
        return pl.ds(pl.multiple_of(j * blk, blk), blk)

    @pl.when(i == 0)
    def _():
        def fill(j, c):
            sl = rows(j)
            kt_ref[:, sl] = k_ref[sl, :].T
            vt_ref[:, sl] = v_ref[sl, :].T
            dk_ref[sl, :] = jnp.zeros((blk, head_dim), f32)
            dv_ref[sl, :] = jnp.zeros((blk, head_dim), f32)
            return c
        lax.fori_loop(0, n_blk, fill, 0)

    q = q_ref[...]
    do = do_ref[...]

    def lanes(col):
        return jnp.concatenate([col] * (blk // col.shape[1]), axis=1)

    def pass_a(j, mx, diag):
        sl = rows(j)
        s = lax.dot_general(k_ref[sl, :], q, nt, preferred_element_type=f32)
        row = lax.broadcasted_iota(jnp.int32, (blk, 128), 0)
        gap = (row + (j - i) * blk).astype(f32) * slope2
        s = s * (scale * log2e) + lanes(gap)
        if diag:
            key = lax.broadcasted_iota(jnp.int32, (blk, blk), 0)
            qry = lax.broadcasted_iota(jnp.int32, (blk, blk), 1)
            s = jnp.where(key <= qry, s, -1e30)
        s_ref[sl, :] = s
        dp_ref[sl, :] = lax.dot_general(v_ref[sl, :], do, nt, preferred_element_type=f32)
        return jnp.maximum(mx, jnp.max(s.reshape(blk // 8, 8, blk), axis=0))

    mx = lax.fori_loop(0, i, lambda j, c: pass_a(j, c, False), jnp.full((8, blk), -1e30, f32))
    mx = pass_a(i, mx, True)
    mx = jnp.max(mx, axis=0, keepdims=True)

    acc_ref[...] = jnp.zeros(acc_ref.shape, f32)

    def pass_b(j, c):
        tot, dlt = c
        sl = rows(j)
        p = jnp.exp2(s_ref[sl, :] - mx)
        s_ref[sl, :] = p
        acc_ref[...] += jnp.dot(vt_ref[:, sl], p.astype(bf16), preferred_element_type=f32)
        tot = tot + jnp.sum(p.reshape(blk // 8, 8, blk), axis=0)
        dlt = dlt + jnp.sum((p * dp_ref[sl, :]).reshape(blk // 8, 8, blk), axis=0)
        return tot, dlt

    zero = jnp.zeros((8, blk), f32)
    tot, dlt = lax.fori_loop(0, i + 1, pass_b, (zero, zero))
    inv = 1.0 / jnp.sum(tot, axis=0, keepdims=True)
    dlt = jnp.sum(dlt, axis=0, keepdims=True) * inv
    n_tok = blk // tok
    o_blk = (acc_ref[...] * inv).T.astype(bf16)
    for t in range(n_tok):
        out_ref[i * n_tok + t, 0] = o_blk[t * tok:(t + 1) * tok]

    acc_ref[...] = jnp.zeros(acc_ref.shape, f32)

    def pass_c(j, c):
        sl = rows(j)
        p = s_ref[sl, :] * inv
        dv_ref[sl, :] += jnp.dot(p.astype(bf16), do, preferred_element_type=f32)
        ds = (p * (dp_ref[sl, :] - dlt)).astype(bf16)
        dk_ref[sl, :] += jnp.dot(ds, q, preferred_element_type=f32)
        acc_ref[...] += jnp.dot(kt_ref[:, sl], ds, preferred_element_type=f32)
        return c

    lax.fori_loop(0, i + 1, pass_c, 0)
    dq_blk = (acc_ref[...] * scale).T.astype(bf16)
    for t in range(n_tok):
        out_ref[i * n_tok + t, 1] = dq_blk[t * tok:(t + 1) * tok]

    @pl.when(i == n_blk - 1)
    def _():
        for t in range(n_blk * n_tok):
            out_ref[t, 2] = (dk_ref[t * tok:(t + 1) * tok, :] * scale).astype(bf16)
            out_ref[t, 3] = dv_ref[t * tok:(t + 1) * tok, :].astype(bf16)


def attention(q, k, v, do, slope, tok, blk=512):
    seq, head_dim = q.shape
    n_blk = seq // blk
    full = pl.BlockSpec((seq, head_dim), lambda i: (0, 0))
    part = pl.BlockSpec((blk, head_dim), lambda i: (i, 0))
    pairs = seq * (seq + blk) // 2
    f32, bf16 = jnp.float32, jnp.bfloat16
    return pl.pallas_call(
        functools.partial(attn_kernel, blk, tok),
        grid=(n_blk,),
        out_shape=jax.ShapeDtypeStruct((seq // tok, 4, tok, head_dim), bf16),
        in_specs=[pl.BlockSpec(memory_space=pltpu.SMEM), part, full, full, part],
        out_specs=pl.BlockSpec((seq // tok, 4, tok, head_dim), lambda i: (0, 0, 0, 0)),
        scratch_shapes=[
            pltpu.VMEM((head_dim, seq), bf16), pltpu.VMEM((head_dim, seq), bf16),
            pltpu.VMEM((seq, blk), f32), pltpu.VMEM((seq, blk), f32),
            pltpu.VMEM((seq, head_dim), f32), pltpu.VMEM((seq, head_dim), f32),
            pltpu.VMEM((head_dim, blk), f32),
        ],
        compiler_params=pltpu.CompilerParams(dimension_semantics=("arbitrary",), vmem_limit_bytes=56 * 2 ** 20),
        cost_estimate=pl.CostEstimate(flops=12 * pairs * head_dim * 2, bytes_accessed=8 * seq * head_dim * 2, transcendentals=pairs),
        name="attn_fwd_bwd",
    )(slope, q, k, v, do)


def alibi_slopes(n_heads):
    pow_two = 2 ** math.ceil(math.log2(n_heads))
    exponents = jnp.arange(1, pow_two + 1, dtype=jnp.float32) * (8.0 / pow_two)
    slopes = jnp.exp2(-exponents)
    if pow_two != n_heads:
        slopes = jnp.concatenate([slopes[1::2], slopes[0::2]])[:n_heads]
    return slopes


def layer_norm(values, weight):
    centered = values - jnp.mean(values, axis=-1, keepdims=True)
    var_val = jnp.mean(centered * centered, axis=-1, keepdims=True)
    return centered * lax.rsqrt(var_val + 1e-5) * weight


def head_stats(raw):
    mean = jnp.mean(raw, axis=(0, 2))
    centered = raw - mean[None, :, None]
    return mean, lax.rsqrt(jnp.mean(centered * centered, axis=(0, 2)) + 1e-5)


def solution(mesh):
    n_sp = mesh.shape['sp']
    seq_spec = P(None, 'sp', None)
    rep_spec = P()

    def local_step(x, ln1_w, w_qkv, q_ln_w, k_ln_w, w_out, grad_y):
        f32, bf16 = jnp.float32, jnp.bfloat16
        n_batch, tok, d_model = x.shape
        n_heads, head_dim = q_ln_w.shape
        assert n_heads == n_sp
        seq = tok * n_sp
        me = lax.axis_index('sp')
        slope = lax.dynamic_slice_in_dim(alibi_slopes(n_heads), me, 1)
        w_out3 = w_out.reshape(n_heads, head_dim, d_model)
        w_qkv4 = w_qkv.reshape(d_model, 3, n_heads, head_dim)
        w_head = lax.dynamic_slice_in_dim(w_qkv4, me, 1, axis=2).reshape(d_model, 3 * head_dim)
        ln_w3 = (q_ln_w.astype(f32)[:, None, :], k_ln_w.astype(f32)[:, None, :])
        ln_head = tuple(lax.dynamic_slice_in_dim(w.astype(f32), me, 1, axis=0) for w in (q_ln_w, k_ln_w))
        x_f32 = x.astype(f32)
        ln1_f32 = ln1_w.astype(f32)

        h_act, h_all = [], []
        for b in range(n_batch):
            h_act.append(layer_norm(x_f32[b], ln1_f32).astype(bf16))
            h_all.append(lax.all_gather(h_act[b], 'sp', axis=0, tiled=True))

        do_head = []
        for b in range(n_batch):
            d_o = jnp.einsum('te,hde->htd', grad_y[b], w_out3, preferred_element_type=f32).astype(bf16)
            do_head.append(lax.all_to_all(d_o, 'sp', 0, 0, tiled=True).reshape(seq, head_dim))

        raw_tok, stats_tok = [], []
        for b in range(n_batch):
            raw = [jnp.einsum('te,ehd->htd', h_act[b], w_qkv4[:, n], preferred_element_type=f32) for n in range(2)]
            raw_tok.append(raw)
            stats_tok.append([head_stats(r) for r in raw])
        stats = jnp.stack([jnp.stack([s for pair in st for s in pair]) for st in stats_tok])
        stats_all = lax.all_gather(stats, 'sp')
        stats_all = jnp.moveaxis(stats_all, 0, 2).reshape(n_batch, 4, seq)

        outs, back, xhat = [], [], []
        for b in range(n_batch):
            raw = jnp.dot(h_all[b], w_head, preferred_element_type=f32)
            hat = [(raw[:, n * head_dim:(n + 1) * head_dim] - stats_all[b, 2 * n][:, None]) * stats_all[b, 2 * n + 1][:, None] for n in range(2)]
            xhat.append(hat)
            q, k = [(hat[n] * ln_head[n]).astype(bf16) for n in range(2)]
            v = raw[:, 2 * head_dim:].astype(bf16)
            out = attention(q, k, v, do_head[b], slope, tok)
            outs.append(out)
            back.append(lax.all_to_all(out, 'sp', 0, 0, tiled=True))

        o_tok = jnp.stack([t[:, 0] for t in back])
        grad_w_out = lax.psum(jnp.einsum('bhtd,bte->hde', o_tok, grad_y, preferred_element_type=f32).reshape(d_model, d_model), 'sp')

        y, grad_x, means, ln_grads = [], [], [], []
        for b in range(n_batch):
            t = back[b]
            y.append((jnp.einsum('htd,hde->te', t[:, 0], w_out3, preferred_element_type=f32) + x_f32[b]).astype(bf16))
            parts, mean_b, ln_b = [], [], []
            for n in range(2):
                mean, rstd = stats_tok[b][n]
                hat = (raw_tok[b][n] - mean[None, :, None]) * rstd[None, :, None]
                g = t[:, 1 + n].astype(f32)
                gw = g * ln_w3[n]
                c1 = jnp.mean(gw, axis=(0, 2))
                c2 = jnp.mean(gw * hat, axis=(0, 2))
                mean_b += [c1, c2]
                ln_b.append(jnp.sum(g * hat, axis=1))
                parts.append(((gw - c1[None, :, None] - hat * c2[None, :, None]) * rstd[None, :, None]).astype(bf16))
            parts.append(t[:, 3])
            means.append(jnp.stack(mean_b))
            d_qkv = jnp.concatenate(parts, axis=0)
            d_h = jnp.einsum('ctd,ecd->te', d_qkv, w_qkv.reshape(d_model, 3 * n_heads, head_dim), preferred_element_type=f32).astype(bf16)
            _, ln1_pull = jax.vjp(layer_norm, x_f32[b], ln1_f32)
            d_x, g_ln1 = ln1_pull(d_h.astype(f32))
            ln_grads.append((g_ln1, ln_b[0], ln_b[1]))
            grad_x.append((d_x + grad_y[b].astype(f32)).astype(bf16))

        means_all = jnp.moveaxis(lax.all_gather(jnp.stack(means), 'sp'), 0, 2).reshape(n_batch, 4, seq)

        def w_grad(cols):
            total = sum(lax.dot_general(h_all[b], cols[b], (((0,), (0,)), ((), ())), preferred_element_type=f32) for b in range(n_batch))
            return lax.all_gather(total, 'sp')

        pieces = [w_grad([outs[b][:, 3].reshape(seq, head_dim) for b in range(n_batch)])]
        for n in (1, 0):
            cols = []
            for b in range(n_batch):
                gw = outs[b][:, 1 + n].reshape(seq, head_dim).astype(f32) * ln_head[n]
                rstd = stats_all[b, 2 * n + 1][:, None]
                cols.append(((gw - means_all[b, 2 * n][:, None] - xhat[b][n] * means_all[b, 2 * n + 1][:, None]) * rstd).astype(bf16))
            pieces.append(w_grad(cols))
        grad_w_qkv = jnp.concatenate([jnp.moveaxis(p, 0, 1).reshape(d_model, d_model) for p in pieces[::-1]], axis=1)

        small = lax.psum(tuple(sum(g[m] for g in ln_grads) for m in range(3)), 'sp')
        return (jnp.stack(y), jnp.stack(grad_x), small[0], grad_w_qkv, small[1], small[2], grad_w_out)

    return jax.shard_map(local_step, mesh=mesh, in_specs=(seq_spec, rep_spec, rep_spec, rep_spec, rep_spec, rep_spec, seq_spec), out_specs=(seq_spec, seq_spec, rep_spec, rep_spec, rep_spec, rep_spec, rep_spec), check_vma=False)
```

```python
import functools, math
import jax
import jax.numpy as jnp
from jax import lax
from jax.experimental import pallas as pl
from jax.experimental.pallas import tpu as pltpu
from jax.sharding import PartitionSpec as P

def flip(me, off, n_dev):
    res, bit = 0, 1
    while bit < n_dev:
        res = res + lax.rem(me // bit + off // bit % 2, 2) * bit
        bit *= 2
    return res


def meet(n_dev, bits):
    me = lax.axis_index('sp')
    barrier = pltpu.get_barrier_semaphore()
    for bit in bits:
        pl.semaphore_signal(barrier, inc=1, device_id=(flip(me, bit, n_dev),), device_id_type=pl.DeviceIdType.MESH)
    pl.semaphore_wait(barrier, len(bits))


def span(bits):
    res = [0]
    for bit in bits:
        res = res + [off ^ bit for off in res]
    return res


def reduce_plan(n_dev):
    dims = []
    bit = 2
    while bit < n_dev:
        dims.append(bit)
        bit *= 2
    return [[1] + dims[c:] + dims[:c] for c in range(len(dims))]


def scatter_kernel(n_dev, part_ref, dst_ref, acc_ref, recv_ref, rs_send, rs_recv, loc_sem, out_sem):
    me = lax.axis_index('sp')
    rows = part_ref.shape[1]
    orders = reduce_plan(n_dev)
    n_col = len(orders)
    lanes = part_ref.shape[2] // 128
    cuts = [lanes * c // n_col * 128 for c in range(n_col + 1)]
    ids = {}
    for c, order in enumerate(orders):
        for t in range(len(order)):
            for off in span(order[t + 1:]):
                ids[(c, t, off)] = len(ids)

    def block(off):
        return flip(me, off, n_dev) // 2

    def load(off):
        d = flip(me, off, n_dev)
        return pltpu.make_async_copy(part_ref.at[d], acc_ref.at[d // 2], loc_sem.at[off // 2])

    def copy(key):
        c, t, off = key
        bit = orders[c][t]
        cols = pl.ds(cuts[c], cuts[c + 1] - cuts[c])
        k = ids[key]
        src = part_ref.at[flip(me, bit ^ off, n_dev), :, cols] if t == 0 else acc_ref.at[block(bit ^ off), :, cols]
        return pltpu.make_async_remote_copy(src_ref=src, dst_ref=recv_ref.at[k, :, pl.ds(0, cuts[c + 1] - cuts[c])],
                                            send_sem=rs_send.at[k], recv_sem=rs_recv.at[k], device_id=(flip(me, bit, n_dev),), device_id_type=pl.DeviceIdType.MESH)

    def add(key):
        c, t, off = key
        copy(key).wait_recv()
        cols = pl.ds(cuts[c], cuts[c + 1] - cuts[c])
        acc_ref[block(off), :, cols] = acc_ref[block(off), :, cols] + recv_ref[ids[key], :, 0:cuts[c + 1] - cuts[c]]

    bits = [1]
    while bits[-1] * 2 < n_dev:
        bits.append(bits[-1] * 2)
    for off in range(0, n_dev, 2):
        load(off).start()
    meet(n_dev, bits)
    n_step = len(orders[0])
    for t in range(n_step):
        if t == 0:
            for c in range(n_col):
                for off in span(orders[c][1:]):
                    copy((c, 0, off)).start()
            for off in range(0, n_dev, 2):
                load(off).wait()
            continue
        for c in range(n_col):
            bit = orders[c][t]
            for off in span(orders[c][t + 1:]):
                add((c, t - 1, off ^ bit))
                copy((c, t, off)).start()
        for c in range(n_col):
            for off in span(orders[c][t + 1:]):
                add((c, t - 1, off))
    for c in range(n_col):
        add((c, n_step - 1, 0))

    def own(j):
        return pltpu.make_async_copy(acc_ref.at[block(0), :, pl.ds(j * 128, 128)], dst_ref.at[j], out_sem.at[j])

    for j in range(lanes):
        own(j).start()
    for key in ids:
        copy(key).wait_send()
    for j in range(lanes):
        own(j).wait()


def reduce_scatter(part, n_dev, call_id):
    n_row, n_col = part.shape
    rows = n_row // n_dev
    orders = reduce_plan(n_dev)
    n = sum(len(span(order[t + 1:])) for order in orders for t in range(len(order)))
    width = (n_col // 128 + len(orders) - 1) // len(orders) * 128
    sems = pltpu.SemaphoreType.DMA((n,))
    return pl.pallas_call(
        functools.partial(scatter_kernel, n_dev),
        out_shape=jax.ShapeDtypeStruct((n_col // 128, rows, 128), part.dtype),
        in_specs=[pl.BlockSpec(memory_space=pl.ANY)],
        out_specs=pl.BlockSpec(memory_space=pl.ANY),
        scratch_shapes=[pltpu.VMEM((n_dev // 2, rows, n_col), part.dtype), pltpu.VMEM((n, rows, width), part.dtype), sems, sems, pltpu.SemaphoreType.DMA((n_dev // 2,)), pltpu.SemaphoreType.DMA((n_col // 128,))],
        compiler_params=pltpu.CompilerParams(collective_id=call_id, has_side_effects=True, vmem_limit_bytes=32 * 2 ** 20),
        cost_estimate=pl.CostEstimate(flops=10 ** 7, bytes_accessed=part.size * 8, transcendentals=0),
        name="sum_scatter",
    )(part.reshape(n_dev, rows, n_col))


def attn_kernel(blk, tok, n_dev, n_src, slope_ref, q_ref, k_ref, v_ref, do_ref, *refs):
    src_refs, out_ref, dst_refs = refs[:n_src], refs[n_src], refs[n_src + 1:2 * n_src + 1]
    kt_ref, vt_ref, s_ref, dp_ref, dk_ref, dv_ref, acc_ref, send_sem, recv_sem, loc_sem = refs[2 * n_src + 1:]
    i = pl.program_id(0)
    n_blk = pl.num_programs(0)
    me = lax.axis_index('sp')

    def send(j, off):
        peer = flip(me, off, n_dev)
        return pltpu.make_async_remote_copy(src_ref=src_refs[j].at[peer], dst_ref=dst_refs[j].at[me], send_sem=send_sem.at[j, off], recv_sem=recv_sem.at[j, off], device_id=(peer,), device_id_type=pl.DeviceIdType.MESH)

    def keep(j):
        return pltpu.make_async_copy(src_refs[j].at[me], dst_refs[j].at[me], loc_sem.at[j])

    @pl.when(i == 0)
    def _():
        barrier = pltpu.get_barrier_semaphore()
        for off in range(1, n_dev):
            pl.semaphore_signal(barrier, inc=1, device_id=(flip(me, off, n_dev),), device_id_type=pl.DeviceIdType.MESH)
        pl.semaphore_wait(barrier, n_dev - 1)
        for j in range(n_src):
            for off in range(1, n_dev):
                send(j, off).start()
            keep(j).start()

    head_dim = q_ref.shape[1]
    f32, bf16 = jnp.float32, jnp.bfloat16
    scale = head_dim ** -0.5
    log2e = math.log2(math.e)
    slope2 = slope_ref[0] * log2e
    nt = (((1,), (1,)), ((), ()))

    def rows(j):
        return pl.ds(pl.multiple_of(j * blk, blk), blk)

    @pl.when(i == 0)
    def _():
        def fill(j, c):
            sl = rows(j)
            kt_ref[:, sl] = k_ref[sl, :].T
            vt_ref[:, sl] = v_ref[sl, :].T
            dk_ref[sl, :] = jnp.zeros((blk, head_dim), f32)
            dv_ref[sl, :] = jnp.zeros((blk, head_dim), f32)
            return c
        lax.fori_loop(0, n_blk, fill, 0)

    q = q_ref[...]
    do = do_ref[...]

    def lanes(col):
        return jnp.concatenate([col] * (blk // col.shape[1]), axis=1)

    def pass_a(j, mx, diag):
        sl = rows(j)
        s = lax.dot_general(k_ref[sl, :], q, nt, preferred_element_type=f32)
        row = lax.broadcasted_iota(jnp.int32, (blk, 128), 0)
        gap = (row + (j - i) * blk).astype(f32) * slope2
        s = s * (scale * log2e) + lanes(gap)
        if diag:
            key = lax.broadcasted_iota(jnp.int32, (blk, blk), 0)
            qry = lax.broadcasted_iota(jnp.int32, (blk, blk), 1)
            s = jnp.where(key <= qry, s, -1e30)
        s_ref[sl, :] = s
        dp_ref[sl, :] = lax.dot_general(v_ref[sl, :], do, nt, preferred_element_type=f32)
        return jnp.maximum(mx, jnp.max(s.reshape(blk // 8, 8, blk), axis=0))

    mx = lax.fori_loop(0, i, lambda j, c: pass_a(j, c, False), jnp.full((8, blk), -1e30, f32))
    mx = pass_a(i, mx, True)
    mx = jnp.max(mx, axis=0, keepdims=True)

    acc_ref[...] = jnp.zeros(acc_ref.shape, f32)

    def pass_b(j, c):
        tot, dlt = c
        sl = rows(j)
        p = jnp.exp2(s_ref[sl, :] - mx)
        s_ref[sl, :] = p
        acc_ref[...] += jnp.dot(vt_ref[:, sl], p.astype(bf16), preferred_element_type=f32)
        tot = tot + jnp.sum(p.reshape(blk // 8, 8, blk), axis=0)
        dlt = dlt + jnp.sum((p * dp_ref[sl, :]).reshape(blk // 8, 8, blk), axis=0)
        return tot, dlt

    zero = jnp.zeros((8, blk), f32)
    tot, dlt = lax.fori_loop(0, i + 1, pass_b, (zero, zero))
    inv = 1.0 / jnp.sum(tot, axis=0, keepdims=True)
    dlt = jnp.sum(dlt, axis=0, keepdims=True) * inv
    n_tok = blk // tok
    o_blk = (acc_ref[...] * inv).T.astype(bf16)
    for t in range(n_tok):
        out_ref[i * n_tok + t, 0] = o_blk[t * tok:(t + 1) * tok]

    acc_ref[...] = jnp.zeros(acc_ref.shape, f32)

    def pass_c(j, c):
        sl = rows(j)
        p = s_ref[sl, :] * inv
        dv_ref[sl, :] += jnp.dot(p.astype(bf16), do, preferred_element_type=f32)
        ds = (p * (dp_ref[sl, :] - dlt)).astype(bf16)
        dk_ref[sl, :] += jnp.dot(ds, q, preferred_element_type=f32)
        acc_ref[...] += jnp.dot(kt_ref[:, sl], ds, preferred_element_type=f32)
        return c

    lax.fori_loop(0, i + 1, pass_c, 0)
    dq_blk = (acc_ref[...] * scale).T.astype(bf16)
    for t in range(n_tok):
        out_ref[i * n_tok + t, 1] = dq_blk[t * tok:(t + 1) * tok]

    @pl.when(i == n_blk - 1)
    def _():
        for t in range(n_blk * n_tok):
            out_ref[t, 2] = (dk_ref[t * tok:(t + 1) * tok, :] * scale).astype(bf16)
            out_ref[t, 3] = dv_ref[t * tok:(t + 1) * tok, :].astype(bf16)
        for j in range(n_src):
            keep(j).wait()
            for off in range(1, n_dev):
                send(j, off).wait()


def attention(q, k, v, do, slope, tok, srcs, call_id, blk=512):
    n_src, n_dev = len(srcs), srcs[0].shape[0]
    hbm = pl.BlockSpec(memory_space=pl.ANY)
    sems = pltpu.SemaphoreType.DMA((n_src, n_dev))
    seq, head_dim = q.shape
    n_blk = seq // blk
    full = pl.BlockSpec((seq, head_dim), lambda i: (0, 0))
    part = pl.BlockSpec((blk, head_dim), lambda i: (i, 0))
    pairs = seq * (seq + blk) // 2
    f32, bf16 = jnp.float32, jnp.bfloat16
    return pl.pallas_call(
        functools.partial(attn_kernel, blk, tok, n_dev, n_src),
        grid=(n_blk,),
        out_shape=[jax.ShapeDtypeStruct((seq // tok, 4, tok, head_dim), bf16)] + [jax.ShapeDtypeStruct(src.shape, src.dtype) for src in srcs],
        in_specs=[pl.BlockSpec(memory_space=pltpu.SMEM), part, full, full, part] + [hbm] * n_src,
        out_specs=[pl.BlockSpec((seq // tok, 4, tok, head_dim), lambda i: (0, 0, 0, 0))] + [hbm] * n_src,
        scratch_shapes=[
            pltpu.VMEM((head_dim, seq), bf16), pltpu.VMEM((head_dim, seq), bf16),
            pltpu.VMEM((seq, blk), f32), pltpu.VMEM((seq, blk), f32),
            pltpu.VMEM((seq, head_dim), f32), pltpu.VMEM((seq, head_dim), f32),
            pltpu.VMEM((head_dim, blk), f32),
            sems, sems, pltpu.SemaphoreType.DMA((n_src,)),
        ],
        compiler_params=pltpu.CompilerParams(dimension_semantics=("arbitrary",), vmem_limit_bytes=56 * 2 ** 20, collective_id=call_id, has_side_effects=True),
        cost_estimate=pl.CostEstimate(flops=12 * pairs * head_dim * 2, bytes_accessed=8 * seq * head_dim * 2, transcendentals=pairs),
        name="attn_fwd_bwd",
    )(slope, q, k, v, do, *srcs)


def place_kernel(n_grp, width, piece_ref, *refs):
    out_ref = refs[-1]
    n_dev = piece_ref.shape[0]
    for g in range(n_grp):
        for d in range(n_dev):
            out_ref[:, (g * n_dev + d) * width:(g * n_dev + d + 1) * width] = piece_ref[d, :, g * width:(g + 1) * width]


def place(piece, whole, col, n_grp, n_col, rows=256):
    n_dev, n_row, width = piece.shape
    width //= n_grp
    in_specs = [pl.BlockSpec((n_dev, rows, n_grp * width), lambda i: (0, i, 0))]
    args = [piece]
    if whole is not None:
        in_specs.append(pl.BlockSpec(memory_space=pl.ANY))
        args.append(whole)
    return pl.pallas_call(
        functools.partial(place_kernel, n_grp, width),
        grid=(n_row // rows,),
        out_shape=jax.ShapeDtypeStruct((n_row, n_col * n_dev * width), piece.dtype),
        in_specs=in_specs,
        out_specs=pl.BlockSpec((rows, n_grp * n_dev * width), lambda i: (i, col)),
        input_output_aliases={} if whole is None else {1: 0},
        compiler_params=pltpu.CompilerParams(dimension_semantics=("arbitrary",)),
        cost_estimate=pl.CostEstimate(flops=piece.size * 16, bytes_accessed=piece.size * 8, transcendentals=0),
        name="place_cols",
    )(*args)


def rows_kernel(piece_ref, out_ref):
    for j in range(piece_ref.shape[1]):
        out_ref[:, j * 128:(j + 1) * 128] = piece_ref[0, j]


def join_rows(piece):
    n_dev, lanes, rows, _ = piece.shape
    return pl.pallas_call(
        rows_kernel,
        grid=(n_dev,),
        out_shape=jax.ShapeDtypeStruct((n_dev * rows, lanes * 128), piece.dtype),
        in_specs=[pl.BlockSpec((1, lanes, rows, 128), lambda i: (i, 0, 0, 0))],
        out_specs=pl.BlockSpec((rows, lanes * 128), lambda i: (i, 0)),
        compiler_params=pltpu.CompilerParams(dimension_semantics=("arbitrary",)),
        cost_estimate=pl.CostEstimate(flops=piece.size * 16, bytes_accessed=piece.size * 8, transcendentals=0),
        name="join_rows",
    )(piece)


def alibi_slopes(n_heads):
    pow_two = 2 ** math.ceil(math.log2(n_heads))
    exponents = jnp.arange(1, pow_two + 1, dtype=jnp.float32) * (8.0 / pow_two)
    slopes = jnp.exp2(-exponents)
    if pow_two != n_heads:
        slopes = jnp.concatenate([slopes[1::2], slopes[0::2]])[:n_heads]
    return slopes


def layer_norm(values, weight):
    centered = values - jnp.mean(values, axis=-1, keepdims=True)
    var_val = jnp.mean(centered * centered, axis=-1, keepdims=True)
    return centered * lax.rsqrt(var_val + 1e-5) * weight


def row_stats(raw):
    mean = jnp.mean(raw, axis=-1)
    centered = raw - mean[..., None]
    return mean, lax.rsqrt(jnp.mean(centered * centered, axis=-1) + 1e-5)


def solution(mesh):
    n_sp = mesh.shape['sp']
    seq_spec = P(None, 'sp', None)
    rep_spec = P()

    def local_step(x, ln1_w, w_qkv, q_ln_w, k_ln_w, w_out, grad_y):
        f32, bf16 = jnp.float32, jnp.bfloat16
        n_batch, tok, d_model = x.shape
        n_heads, head_dim = q_ln_w.shape
        assert n_heads == n_sp and n_batch == 3
        seq = tok * n_sp
        me = lax.axis_index('sp')
        slope = lax.dynamic_slice_in_dim(alibi_slopes(n_heads), me, 1)
        w_head = jnp.concatenate([lax.dynamic_slice_in_dim(w_qkv, n * d_model + me * head_dim, head_dim, axis=1) for n in range(3)], axis=1)
        ln_flat = [w.reshape(d_model).astype(f32) for w in (q_ln_w, k_ln_w)]
        ln_head = [lax.dynamic_slice_in_dim(w.astype(f32), me, 1, axis=0) for w in (q_ln_w, k_ln_w)]
        x_f32 = x.astype(f32)
        ln1_f32 = ln1_w.astype(f32)

        h_act = layer_norm(x_f32, ln1_f32).astype(bf16)
        h_all = [lax.all_gather(h_act[b], 'sp', axis=0, tiled=True) for b in range(n_batch)]

        d_o = jnp.einsum('bte,fe->btf', grad_y, w_out, preferred_element_type=f32).astype(bf16)
        d_o = jnp.moveaxis(d_o.reshape(n_batch, tok, n_heads, head_dim), 2, 0)
        do_first = lax.all_to_all(d_o[:, 0], 'sp', 0, 0, tiled=True).reshape(seq, head_dim)

        raw_tok = jnp.einsum('bte,ef->btf', h_act, w_qkv[:, :2 * d_model], preferred_element_type=f32)
        stats_tok = [row_stats(raw_tok[..., n * d_model:(n + 1) * d_model]) for n in range(2)]
        stats_all = lax.all_gather(jnp.stack([s for pair in stats_tok for s in pair]), 'sp')
        stats_all = jnp.moveaxis(stats_all, 0, 2).reshape(4, n_batch, seq)

        def grow(b, col):
            return lax.dot_general(h_all[b], col, (((0,), (0,)), ((), ())), preferred_element_type=f32)

        outs, back, xhat = [], [], []
        dv_part, d_head = None, [do_first]
        for b in range(n_batch):
            if b == n_batch - 1:
                dv_part = sum(grow(a, outs[a][:, 3].reshape(seq, head_dim)) for a in range(b))
            if b > 0:
                w_head, outs[-1], dv_part = lax.optimization_barrier((w_head, outs[-1], dv_part))
            raw = jnp.dot(h_all[b], w_head, preferred_element_type=f32)
            hat = [(raw[:, n * head_dim:(n + 1) * head_dim] - stats_all[2 * n, b][:, None]) * stats_all[2 * n + 1, b][:, None] for n in range(2)]
            xhat.append(hat)
            q, k = [(hat[n] * ln_head[n]).astype(bf16) for n in range(2)]
            v = raw[:, 2 * head_dim:].astype(bf16)
            srcs = [d_o[:, a] for a in range(1, n_batch)] if b == 0 else [outs[-1].reshape(n_heads, 4 * tok, head_dim)]
            out, *got = attention(q, k, v, d_head[b], slope, tok, srcs, b)
            if b == 0:
                d_head += [t.reshape(seq, head_dim) for t in got]
            else:
                back.append(got[0].reshape(n_heads, 4, tok, head_dim))
            outs.append(out)
        back.append(lax.all_to_all(outs[-1], 'sp', 0, 0, tiled=True))

        grad_v = dv_part + grow(n_batch - 1, outs[-1][:, 3].reshape(seq, head_dim))
        back[-1], grad_v = lax.optimization_barrier((back[-1], grad_v))
        grad_v = lax.all_gather(grad_v, 'sp')

        def natural(lo, hi):
            return [jnp.stack([jnp.moveaxis(t[:, n], 0, 1).reshape(tok, d_model) for t in back[lo:hi]]) for n in range(4)]

        def token_means(lo, hi, nat):
            res = []
            for n in range(2):
                hat = (raw_tok[lo:hi, :, n * d_model:(n + 1) * d_model] - stats_tok[n][0][lo:hi, :, None]) * stats_tok[n][1][lo:hi, :, None]
                gw = nat[1 + n].astype(f32) * ln_flat[n]
                res += [jnp.mean(gw, axis=-1), jnp.mean(gw * hat, axis=-1)]
            return jnp.stack(res)

        def first_half(lo, hi, nat, mean):
            y = (jnp.einsum('btd,de->bte', nat[0], w_out, preferred_element_type=f32) + x_f32[lo:hi]).astype(bf16)
            stat = [[s[lo:hi, :, None] for s in pair] for pair in stats_tok]
            hats = [(raw_tok[lo:hi, :, n * d_model:(n + 1) * d_model] - stat[n][0]) * stat[n][1] for n in range(2)]
            grads = [nat[1 + n].astype(f32) for n in range(2)]
            raws = [((grads[n] * ln_flat[n] - mean[2 * n][..., None] - hats[n] * mean[2 * n + 1][..., None]) * stat[n][1]).astype(bf16) for n in range(2)]
            d_qkv = jnp.concatenate(raws + [nat[3]], axis=-1)
            d_h = jnp.einsum('bte,de->btd', d_qkv, w_qkv, preferred_element_type=f32).astype(bf16)
            return y, d_h, [jnp.sum(grads[n] * hats[n], axis=(0, 1)) for n in range(2)]

        def second_half(lo, hi, d_h):
            _, ln1_pull = jax.vjp(layer_norm, x_f32[lo:hi], ln1_f32)
            d_x, grad_ln1 = ln1_pull(d_h.astype(f32))
            return (d_x + grad_y[lo:hi].astype(f32)).astype(bf16), grad_ln1

        last = n_batch - 1
        nat_a = natural(0, last)
        mean_a = token_means(0, last, nat_a)
        nat_b = natural(last, n_batch)
        mean_b = token_means(last, n_batch, nat_b)
        means_all = lax.all_gather(jnp.concatenate([mean_a, mean_b], axis=1), 'sp')
        means_all = jnp.moveaxis(means_all, 0, 2).reshape(4, n_batch, seq)

        total = 0.0
        for b in range(n_batch):
            cols = []
            for n in range(2):
                gw = outs[b][:, 1 + n].reshape(seq, head_dim).astype(f32) * ln_head[n]
                rstd = stats_all[2 * n + 1, b][:, None]
                cols.append(((gw - means_all[2 * n, b][:, None] - xhat[b][n] * means_all[2 * n + 1, b][:, None]) * rstd).astype(bf16))
            total = total + grow(b, jnp.concatenate(cols, axis=1))
        total, grad_v = lax.optimization_barrier((total, grad_v))
        grad_qk = lax.all_gather(total, 'sp')

        o_tok = jnp.concatenate([nat_a[0], nat_b[0]])
        w_out_part = jnp.einsum('btd,bte->de', o_tok, grad_y, preferred_element_type=f32)
        w_out_part, total = lax.optimization_barrier((w_out_part, total))
        w_out_sum = reduce_scatter(w_out_part, n_sp, n_batch)
        nat = [jnp.concatenate(pair) for pair in zip(nat_a, nat_b)]
        mean = jnp.concatenate([mean_a, mean_b], axis=1)
        w_out_sum, nat, mean = lax.optimization_barrier((w_out_sum, nat, mean))
        y, d_h, ln_grads = first_half(0, n_batch, nat, mean)
        w_out_sum, grad_qk, d_h, y = lax.optimization_barrier((w_out_sum, grad_qk, d_h, y))
        w_out_all = lax.all_gather(w_out_sum, 'sp')
        grad_x, grad_ln1 = second_half(0, n_batch, d_h)
        small = jnp.sum(lax.all_gather(jnp.stack([grad_ln1] + ln_grads), 'sp'), axis=0)
        grad_w_qkv = place(grad_v, None, 2, 1, 3)
        grad_w_qkv = place(grad_qk, grad_w_qkv, 0, 2, 3)
        grad_w_out = join_rows(w_out_all)
        return (y, grad_x, small[0], grad_w_qkv, small[1].reshape(n_heads, head_dim), small[2].reshape(n_heads, head_dim), grad_w_out)

    return jax.shard_map(local_step, mesh=mesh, in_specs=(seq_spec, rep_spec, rep_spec, rep_spec, rep_spec, rep_spec, seq_spec), out_specs=(seq_spec, seq_spec, rep_spec, rep_spec, rep_spec, rep_spec, rep_spec), check_vma=False)
```

```python
import functools, math
import jax
import jax.numpy as jnp
from jax import lax
from jax.experimental import pallas as pl
from jax.experimental.pallas import tpu as pltpu
from jax.sharding import PartitionSpec as P


def flip(me, off, n_dev):
    res, bit = 0, 1
    while bit < n_dev:
        res = res + lax.rem(me // bit + off // bit % 2, 2) * bit
        bit *= 2
    return res


def meet(n_dev, bits):
    me = lax.axis_index('sp')
    barrier = pltpu.get_barrier_semaphore()
    for bit in bits:
        pl.semaphore_signal(barrier, inc=1, device_id=(flip(me, bit, n_dev),), device_id_type=pl.DeviceIdType.MESH)
    pl.semaphore_wait(barrier, len(bits))


def span(bits):
    res = [0]
    for bit in bits:
        res = res + [off ^ bit for off in res]
    return res


def reduce_plan(n_dev):
    dims = []
    bit = 2
    while bit < n_dev:
        dims.append(bit)
        bit *= 2
    return [[1] + dims[c:] + dims[:c] for c in range(len(dims))]


def scatter_kernel(n_dev, part_ref, dst_ref, acc_ref, recv_ref, rs_send, rs_recv, loc_sem, out_sem):
    me = lax.axis_index('sp')
    orders = reduce_plan(n_dev)
    n_col = len(orders)
    lanes = part_ref.shape[2] // 128
    cuts = [lanes * c // n_col * 128 for c in range(n_col + 1)]
    ids = {}
    for c, order in enumerate(orders):
        for t in range(len(order)):
            for off in span(order[t + 1:]):
                ids[(c, t, off)] = len(ids)

    def block(off):
        return flip(me, off, n_dev) // 2

    def load(off):
        d = flip(me, off, n_dev)
        return pltpu.make_async_copy(part_ref.at[d], acc_ref.at[d // 2], loc_sem.at[off // 2])

    def copy(key):
        c, t, off = key
        bit = orders[c][t]
        cols = pl.ds(cuts[c], cuts[c + 1] - cuts[c])
        k = ids[key]
        src = part_ref.at[flip(me, bit ^ off, n_dev), :, cols] if t == 0 else acc_ref.at[block(bit ^ off), :, cols]
        return pltpu.make_async_remote_copy(src_ref=src, dst_ref=recv_ref.at[k, :, pl.ds(0, cuts[c + 1] - cuts[c])],
                                            send_sem=rs_send.at[k], recv_sem=rs_recv.at[k], device_id=(flip(me, bit, n_dev),), device_id_type=pl.DeviceIdType.MESH)

    def add(key):
        c, _, off = key
        copy(key).wait_recv()
        cols = pl.ds(cuts[c], cuts[c + 1] - cuts[c])
        acc_ref[block(off), :, cols] = acc_ref[block(off), :, cols] + recv_ref[ids[key], :, 0:cuts[c + 1] - cuts[c]]

    bits = [1]
    while bits[-1] * 2 < n_dev:
        bits.append(bits[-1] * 2)
    for off in range(0, n_dev, 2):
        load(off).start()
    meet(n_dev, bits)
    n_step = len(orders[0])
    for t in range(n_step):
        if t == 0:
            for c in range(n_col):
                for off in span(orders[c][1:]):
                    copy((c, 0, off)).start()
            for off in range(0, n_dev, 2):
                load(off).wait()
            continue
        for c in range(n_col):
            bit = orders[c][t]
            for off in span(orders[c][t + 1:]):
                add((c, t - 1, off ^ bit))
                copy((c, t, off)).start()
        for c in range(n_col):
            for off in span(orders[c][t + 1:]):
                add((c, t - 1, off))
    for c in range(n_col):
        add((c, n_step - 1, 0))

    def own(j):
        return pltpu.make_async_copy(acc_ref.at[block(0), :, pl.ds(j * 128, 128)], dst_ref.at[j], out_sem.at[j])

    for j in range(lanes):
        own(j).start()
    for key in ids:
        copy(key).wait_send()
    for j in range(lanes):
        own(j).wait()


def reduce_scatter(part, n_dev, call_id):
    n_row, n_col = part.shape
    rows = n_row // n_dev
    orders = reduce_plan(n_dev)
    n = sum(len(span(order[t + 1:])) for order in orders for t in range(len(order)))
    width = (n_col // 128 + len(orders) - 1) // len(orders) * 128
    sems = pltpu.SemaphoreType.DMA((n,))
    return pl.pallas_call(
        functools.partial(scatter_kernel, n_dev),
        out_shape=jax.ShapeDtypeStruct((n_col // 128, rows, 128), part.dtype),
        in_specs=[pl.BlockSpec(memory_space=pl.ANY)],
        out_specs=pl.BlockSpec(memory_space=pl.ANY),
        scratch_shapes=[pltpu.VMEM((n_dev // 2, rows, n_col), part.dtype), pltpu.VMEM((n, rows, width), part.dtype), sems, sems, pltpu.SemaphoreType.DMA((n_dev // 2,)), pltpu.SemaphoreType.DMA((n_col // 128,))],
        compiler_params=pltpu.CompilerParams(collective_id=call_id, has_side_effects=True, vmem_limit_bytes=32 * 2 ** 20),
        cost_estimate=pl.CostEstimate(flops=10 ** 7, bytes_accessed=part.size * 8, transcendentals=0),
        name="sum_scatter",
    )(part.reshape(n_dev, rows, n_col))


def attn_kernel(blk, tok, n_dev, n_src, slope_ref, q_ref, k_ref, v_ref, do_ref, *refs):
    src_refs, out_ref, dst_refs = refs[:n_src], refs[n_src], refs[n_src + 1:2 * n_src + 1]
    kt_ref, vt_ref, s_ref, dp_ref, dk_ref, dv_ref, acc_ref, send_sem, recv_sem, loc_sem = refs[2 * n_src + 1:]
    i = pl.program_id(0)
    n_blk = pl.num_programs(0)
    me = lax.axis_index('sp')

    def send(j, off):
        peer = flip(me, off, n_dev)
        return pltpu.make_async_remote_copy(src_ref=src_refs[j].at[peer], dst_ref=dst_refs[j].at[me], send_sem=send_sem.at[j, off], recv_sem=recv_sem.at[j, off], device_id=(peer,), device_id_type=pl.DeviceIdType.MESH)

    def keep(j):
        return pltpu.make_async_copy(src_refs[j].at[me], dst_refs[j].at[me], loc_sem.at[j])

    @pl.when(i == 0)
    def _():
        barrier = pltpu.get_barrier_semaphore()
        for off in range(1, n_dev):
            pl.semaphore_signal(barrier, inc=1, device_id=(flip(me, off, n_dev),), device_id_type=pl.DeviceIdType.MESH)
        pl.semaphore_wait(barrier, n_dev - 1)
        for j in range(n_src):
            for off in range(1, n_dev):
                send(j, off).start()
            keep(j).start()

    head_dim = q_ref.shape[1]
    f32, bf16 = jnp.float32, jnp.bfloat16
    scale = head_dim ** -0.5
    log2e = math.log2(math.e)
    slope2 = slope_ref[0] * log2e
    nt = (((1,), (1,)), ((), ()))

    def rows(j):
        return pl.ds(pl.multiple_of(j * blk, blk), blk)

    @pl.when(i == 0)
    def _():
        def fill(j, c):
            sl = rows(j)
            kt_ref[:, sl] = k_ref[sl, :].T
            vt_ref[:, sl] = v_ref[sl, :].T
            dk_ref[sl, :] = jnp.zeros((blk, head_dim), f32)
            dv_ref[sl, :] = jnp.zeros((blk, head_dim), f32)
            return c

        lax.fori_loop(0, n_blk, fill, 0)

    q = q_ref[...]
    do = do_ref[...]

    def lanes(col):
        return jnp.concatenate([col] * (blk // col.shape[1]), axis=1)

    def pass_a(j, mx, diag):
        sl = rows(j)
        s = lax.dot_general(k_ref[sl, :], q, nt, preferred_element_type=f32)
        row = lax.broadcasted_iota(jnp.int32, (blk, 128), 0)
        gap = (row + (j - i) * blk).astype(f32) * slope2
        s = s * (scale * log2e) + lanes(gap)
        if diag:
            key = lax.broadcasted_iota(jnp.int32, (blk, blk), 0)
            qry = lax.broadcasted_iota(jnp.int32, (blk, blk), 1)
            s = jnp.where(key <= qry, s, -1e30)
        s_ref[sl, :] = s
        dp_ref[sl, :] = lax.dot_general(v_ref[sl, :], do, nt, preferred_element_type=f32)
        return jnp.maximum(mx, jnp.max(s.reshape(blk // 8, 8, blk), axis=0))

    mx = lax.fori_loop(0, i, lambda j, c: pass_a(j, c, False), jnp.full((8, blk), -1e30, f32))
    mx = pass_a(i, mx, True)
    mx = jnp.max(mx, axis=0, keepdims=True)

    acc_ref[...] = jnp.zeros(acc_ref.shape, f32)

    def pass_b(j, c):
        tot, dlt = c
        sl = rows(j)
        p = jnp.exp2(s_ref[sl, :] - mx)
        s_ref[sl, :] = p
        acc_ref[...] += jnp.dot(vt_ref[:, sl], p.astype(bf16), preferred_element_type=f32)
        tot = tot + jnp.sum(p.reshape(blk // 8, 8, blk), axis=0)
        dlt = dlt + jnp.sum((p * dp_ref[sl, :]).reshape(blk // 8, 8, blk), axis=0)
        return tot, dlt

    zero = jnp.zeros((8, blk), f32)
    tot, dlt = lax.fori_loop(0, i + 1, pass_b, (zero, zero))
    inv = 1.0 / jnp.sum(tot, axis=0, keepdims=True)
    dlt = jnp.sum(dlt, axis=0, keepdims=True) * inv
    n_tok = blk // tok
    o_blk = (acc_ref[...] * inv).T.astype(bf16)
    for t in range(n_tok):
        out_ref[i * n_tok + t, 0] = o_blk[t * tok:(t + 1) * tok]

    acc_ref[...] = jnp.zeros(acc_ref.shape, f32)

    def pass_c(j, c):
        sl = rows(j)
        p = s_ref[sl, :] * inv
        dv_ref[sl, :] += jnp.dot(p.astype(bf16), do, preferred_element_type=f32)
        ds = (p * (dp_ref[sl, :] - dlt)).astype(bf16)
        dk_ref[sl, :] += jnp.dot(ds, q, preferred_element_type=f32)
        acc_ref[...] += jnp.dot(kt_ref[:, sl], ds, preferred_element_type=f32)
        return c

    lax.fori_loop(0, i + 1, pass_c, 0)
    dq_blk = (acc_ref[...] * scale).T.astype(bf16)
    for t in range(n_tok):
        out_ref[i * n_tok + t, 1] = dq_blk[t * tok:(t + 1) * tok]

    @pl.when(i == n_blk - 1)
    def _():
        for t in range(n_blk * n_tok):
            out_ref[t, 2] = (dk_ref[t * tok:(t + 1) * tok, :] * scale).astype(bf16)
            out_ref[t, 3] = dv_ref[t * tok:(t + 1) * tok, :].astype(bf16)
        for j in range(n_src):
            keep(j).wait()
            for off in range(1, n_dev):
                send(j, off).wait()


def attention(q, k, v, do, slope, tok, srcs, call_id, blk=512):
    n_src, n_dev = len(srcs), srcs[0].shape[0]
    hbm = pl.BlockSpec(memory_space=pl.ANY)
    sems = pltpu.SemaphoreType.DMA((n_src, n_dev))
    seq, head_dim = q.shape
    n_blk = seq // blk
    full = pl.BlockSpec((seq, head_dim), lambda i: (0, 0))
    part = pl.BlockSpec((blk, head_dim), lambda i: (i, 0))
    pairs = seq * (seq + blk) // 2
    f32, bf16 = jnp.float32, jnp.bfloat16
    return pl.pallas_call(
        functools.partial(attn_kernel, blk, tok, n_dev, n_src),
        grid=(n_blk,),
        out_shape=[jax.ShapeDtypeStruct((seq // tok, 4, tok, head_dim), bf16)] + [jax.ShapeDtypeStruct(src.shape, src.dtype) for src in srcs],
        in_specs=[pl.BlockSpec(memory_space=pltpu.SMEM), part, full, full, part] + [hbm] * n_src,
        out_specs=[pl.BlockSpec((seq // tok, 4, tok, head_dim), lambda i: (0, 0, 0, 0))] + [hbm] * n_src,
        scratch_shapes=[
            pltpu.VMEM((head_dim, seq), bf16), pltpu.VMEM((head_dim, seq), bf16),
            pltpu.VMEM((seq, blk), f32), pltpu.VMEM((seq, blk), f32),
            pltpu.VMEM((seq, head_dim), f32), pltpu.VMEM((seq, head_dim), f32),
            pltpu.VMEM((head_dim, blk), f32),
            sems, sems, pltpu.SemaphoreType.DMA((n_src,)),
        ],
        compiler_params=pltpu.CompilerParams(dimension_semantics=("arbitrary",), vmem_limit_bytes=56 * 2 ** 20, collective_id=call_id, has_side_effects=True),
        cost_estimate=pl.CostEstimate(flops=12 * pairs * head_dim * 2, bytes_accessed=8 * seq * head_dim * 2, transcendentals=pairs),
        name="attn_fwd_bwd",
    )(slope, q, k, v, do, *srcs)


def place_kernel(n_grp, width, piece_ref, *refs):
    out_ref = refs[-1]
    n_dev = piece_ref.shape[0]
    for g in range(n_grp):
        for d in range(n_dev):
            out_ref[:, (g * n_dev + d) * width:(g * n_dev + d + 1) * width] = piece_ref[d, :, g * width:(g + 1) * width]


def place(piece, whole, col, n_grp, n_col, rows=256):
    n_dev, n_row, width = piece.shape
    width //= n_grp
    in_specs = [pl.BlockSpec((n_dev, rows, n_grp * width), lambda i: (0, i, 0))]
    args = [piece]
    if whole is not None:
        in_specs.append(pl.BlockSpec(memory_space=pl.ANY))
        args.append(whole)
    return pl.pallas_call(
        functools.partial(place_kernel, n_grp, width),
        grid=(n_row // rows,),
        out_shape=jax.ShapeDtypeStruct((n_row, n_col * n_dev * width), piece.dtype),
        in_specs=in_specs,
        out_specs=pl.BlockSpec((rows, n_grp * n_dev * width), lambda i: (i, col)),
        input_output_aliases={} if whole is None else {1: 0},
        compiler_params=pltpu.CompilerParams(dimension_semantics=("arbitrary",)),
        cost_estimate=pl.CostEstimate(flops=piece.size * 16, bytes_accessed=piece.size * 8, transcendentals=0),
        name="place_cols",
    )(*args)


def rows_kernel(piece_ref, out_ref):
    n_grp, lanes, rows, _ = piece_ref.shape
    for g in range(n_grp):
        for j in range(lanes):
            out_ref[g * rows:(g + 1) * rows, j * 128:(j + 1) * 128] = piece_ref[g, j]


def join_rows(piece, n_grp=4):
    n_dev, lanes, rows, _ = piece.shape
    return pl.pallas_call(
        rows_kernel,
        grid=(n_dev // n_grp,),
        out_shape=jax.ShapeDtypeStruct((n_dev * rows, lanes * 128), piece.dtype),
        in_specs=[pl.BlockSpec((n_grp, lanes, rows, 128), lambda i: (i, 0, 0, 0))],
        out_specs=pl.BlockSpec((n_grp * rows, lanes * 128), lambda i: (i, 0)),
        compiler_params=pltpu.CompilerParams(dimension_semantics=("arbitrary",)),
        cost_estimate=pl.CostEstimate(flops=piece.size * 16, bytes_accessed=piece.size * 8, transcendentals=0),
        name="join_rows",
    )(piece)


def alibi_slopes(n_heads):
    pow_two = 2 ** math.ceil(math.log2(n_heads))
    exponents = jnp.arange(1, pow_two + 1, dtype=jnp.float32) * (8.0 / pow_two)
    slopes = jnp.exp2(-exponents)
    if pow_two != n_heads:
        slopes = jnp.concatenate([slopes[1::2], slopes[0::2]])[:n_heads]
    return slopes


def layer_norm(values, weight):
    centered = values - jnp.mean(values, axis=-1, keepdims=True)
    var_val = jnp.mean(centered * centered, axis=-1, keepdims=True)
    return centered * lax.rsqrt(var_val + 1e-5) * weight


def row_stats(raw):
    mean = jnp.mean(raw, axis=-1)
    centered = raw - mean[..., None]
    return mean, lax.rsqrt(jnp.mean(centered * centered, axis=-1) + 1e-5)


def solution(mesh):
    n_sp = mesh.shape['sp']
    seq_spec = P(None, 'sp', None)
    rep_spec = P()

    def local_step(x, ln1_w, w_qkv, q_ln_w, k_ln_w, w_out, grad_y):
        f32, bf16 = jnp.float32, jnp.bfloat16
        n_batch, tok, d_model = x.shape
        n_heads, head_dim = q_ln_w.shape
        assert n_heads == n_sp and n_batch == 3
        seq = tok * n_sp
        me = lax.axis_index('sp')
        slope = lax.dynamic_slice_in_dim(alibi_slopes(n_heads), me, 1)
        w_head = jnp.concatenate([lax.dynamic_slice_in_dim(w_qkv, n * d_model + me * head_dim, head_dim, axis=1) for n in range(3)], axis=1)
        ln_flat = [w.reshape(d_model).astype(f32) for w in (q_ln_w, k_ln_w)]
        ln_head = [lax.dynamic_slice_in_dim(w.astype(f32), me, 1, axis=0) for w in (q_ln_w, k_ln_w)]
        x_f32 = x.astype(f32)
        ln1_f32 = ln1_w.astype(f32)

        h_act = layer_norm(x_f32, ln1_f32).astype(bf16)
        h_all = [lax.all_gather(h_act[b], 'sp', axis=0, tiled=True) for b in range(n_batch)]

        d_o = jnp.einsum('bte,fe->btf', grad_y, w_out, preferred_element_type=f32).astype(bf16)
        d_o = jnp.moveaxis(d_o.reshape(n_batch, tok, n_heads, head_dim), 2, 0)
        do_first = lax.all_to_all(d_o[:, 0], 'sp', 0, 0, tiled=True).reshape(seq, head_dim)

        do_rest = d_o[:, 1:].reshape(n_heads, (n_batch - 1) * tok, head_dim)

        raw_tok = jnp.einsum('bte,ef->btf', h_act, w_qkv[:, :2 * d_model], preferred_element_type=f32)
        stats_tok = [row_stats(raw_tok[..., n * d_model:(n + 1) * d_model]) for n in range(2)]
        stats_all = lax.all_gather(jnp.stack([s for pair in stats_tok for s in pair]), 'sp')
        stats_all = jnp.moveaxis(stats_all, 0, 2).reshape(4, n_batch, seq)

        def grow(b, col):
            return lax.dot_general(h_all[b], col, (((0,), (0,)), ((), ())), preferred_element_type=f32)

        outs, back, xhat = [], [], []
        dv_part, d_head = None, [do_first]
        for b in range(n_batch):
            if b == n_batch - 1:
                dv_part = sum(grow(a, outs[a][:, 3].reshape(seq, head_dim)) for a in range(b))
            if b > 0:
                w_head, outs[-1], dv_part = lax.optimization_barrier((w_head, outs[-1], dv_part))
            raw = jnp.dot(h_all[b], w_head, preferred_element_type=f32)
            hat = [(raw[:, n * head_dim:(n + 1) * head_dim] - stats_all[2 * n, b][:, None]) * stats_all[2 * n + 1, b][:, None] for n in range(2)]
            xhat.append(hat)
            q, k = [(hat[n] * ln_head[n]).astype(bf16) for n in range(2)]
            v = raw[:, 2 * head_dim:].astype(bf16)
            srcs = [do_rest] if b == 0 else [outs[-1].reshape(n_heads, 4 * tok, head_dim)]
            out, *got = attention(q, k, v, d_head[b], slope, tok, srcs, b)
            if b == 0:
                got = got[0].reshape(n_heads, n_batch - 1, tok, head_dim)
                d_head += [got[:, a].reshape(seq, head_dim) for a in range(n_batch - 1)]
            else:
                back.append(got[0].reshape(n_heads, 4, tok, head_dim))
            outs.append(out)
        back.append(lax.all_to_all(outs[-1], 'sp', 0, 0, tiled=True))

        grad_v = dv_part + grow(n_batch - 1, outs[-1][:, 3].reshape(seq, head_dim))
        back[-1], grad_v = lax.optimization_barrier((back[-1], grad_v))
        grad_v = lax.all_gather(grad_v, 'sp')

        def natural(lo, hi):
            return [jnp.stack([jnp.moveaxis(t[:, n], 0, 1).reshape(tok, d_model) for t in back[lo:hi]]) for n in range(4)]

        def token_means(lo, hi, nat):
            res = []
            for n in range(2):
                hat = (raw_tok[lo:hi, :, n * d_model:(n + 1) * d_model] - stats_tok[n][0][lo:hi, :, None]) * stats_tok[n][1][lo:hi, :, None]
                gw = nat[1 + n].astype(f32) * ln_flat[n]
                res += [jnp.mean(gw, axis=-1), jnp.mean(gw * hat, axis=-1)]
            return jnp.stack(res)

        def first_half(lo, hi, nat, mean):
            stat = [[s[lo:hi, :, None] for s in pair] for pair in stats_tok]
            hats = [(raw_tok[lo:hi, :, n * d_model:(n + 1) * d_model] - stat[n][0]) * stat[n][1] for n in range(2)]
            grads = [nat[1 + n].astype(f32) for n in range(2)]
            raws = [((grads[n] * ln_flat[n] - mean[2 * n][..., None] - hats[n] * mean[2 * n + 1][..., None]) * stat[n][1]).astype(bf16) for n in range(2)]
            d_qkv = jnp.concatenate(raws + [nat[3]], axis=-1)
            d_h = jnp.einsum('bte,de->btd', d_qkv, w_qkv, preferred_element_type=f32).astype(bf16)
            return d_h, [jnp.sum(grads[n] * hats[n], axis=(0, 1)) for n in range(2)]

        def second_half(lo, hi, d_h):
            _, ln1_pull = jax.vjp(layer_norm, x_f32[lo:hi], ln1_f32)
            d_x, grad_ln1 = ln1_pull(d_h.astype(f32))
            return (d_x + grad_y[lo:hi].astype(f32)).astype(bf16), grad_ln1

        last = n_batch - 1
        nat_a = natural(0, last)
        mean_a = token_means(0, last, nat_a)
        nat_a, mean_a = lax.optimization_barrier((nat_a, mean_a))
        y_a = (jnp.einsum('btd,de->bte', nat_a[0], w_out, preferred_element_type=f32) + x_f32[:last]).astype(bf16)
        nat_b = natural(last, n_batch)
        mean_b = token_means(last, n_batch, nat_b)
        means_all = lax.all_gather(jnp.concatenate([mean_a, mean_b], axis=1), 'sp')
        means_all = jnp.moveaxis(means_all, 0, 2).reshape(4, n_batch, seq)

        total = 0.0
        for b in range(n_batch):
            cols = []
            for n in range(2):
                gw = outs[b][:, 1 + n].reshape(seq, head_dim).astype(f32) * ln_head[n]
                rstd = stats_all[2 * n + 1, b][:, None]
                cols.append(((gw - means_all[2 * n, b][:, None] - xhat[b][n] * means_all[2 * n + 1, b][:, None]) * rstd).astype(bf16))
            total = total + grow(b, jnp.concatenate(cols, axis=1))
        total, grad_v = lax.optimization_barrier((total, grad_v))
        grad_qk = lax.all_gather(total, 'sp')

        o_tok = jnp.concatenate([nat_a[0], nat_b[0]])
        w_out_part = jnp.einsum('btd,bte->de', o_tok, grad_y, preferred_element_type=f32)
        w_out_part, total = lax.optimization_barrier((w_out_part, total))
        w_out_sum = reduce_scatter(w_out_part, n_sp, n_batch)
        nat = [jnp.concatenate(pair) for pair in zip(nat_a, nat_b)]
        mean = jnp.concatenate([mean_a, mean_b], axis=1)
        w_out_sum, nat, mean = lax.optimization_barrier((w_out_sum, nat, mean))
        y_b = (jnp.einsum('btd,de->bte', nat_b[0], w_out, preferred_element_type=f32) + x_f32[last:]).astype(bf16)
        y = jnp.concatenate([y_a, y_b])
        d_h, ln_grads = first_half(0, n_batch, nat, mean)
        w_out_sum, grad_qk, d_h, y = lax.optimization_barrier((w_out_sum, grad_qk, d_h, y))
        w_out_all = lax.all_gather(w_out_sum, 'sp')
        grad_x, grad_ln1 = second_half(0, n_batch, d_h)
        small = jnp.sum(lax.all_gather(jnp.stack([grad_ln1] + ln_grads), 'sp'), axis=0)
        grad_w_qkv = place(grad_v, None, 2, 1, 3)
        grad_w_qkv = place(grad_qk, grad_w_qkv, 0, 2, 3)
        grad_w_out = join_rows(w_out_all)
        return (y, grad_x, small[0], grad_w_qkv, small[1].reshape(n_heads, head_dim), small[2].reshape(n_heads, head_dim), grad_w_out)

    return jax.shard_map(local_step, mesh=mesh, in_specs=(seq_spec, rep_spec, rep_spec, rep_spec, rep_spec, rep_spec, seq_spec), out_specs=(seq_spec, seq_spec, rep_spec, rep_spec, rep_spec, rep_spec, rep_spec), check_vma=False)
```
